32 devices in a mesh: site: 8 (over z, y), ka: 4 (over x, core).
Axes of the slice: x: 2, y: 2, z: 4, core: 2. Of those that a mesh axis runs over, the one named last changes fastest.
Arguments:
- positions: float32 [3, 128], P(None, 'site'), may hold values from 0 to 1
- site_class: int32 [128], P('site'), may hold values from 0 to 3
- class_charge: float32 [4], replicated, may hold values from -2 to 2
- miller: int32 [3, 524288], P(None, 'ka'), may hold values from -80 to 80, as said below
Outputs:
- forces: float32 [3, 128], P(None, ('site', 'ka'))
- energy: float32 [], replicated
The draws below stay inside these ranges and needn't reach their ends.
Inputs may be any that keep to these rules, and one draw needn't show every extreme that they name: `miller`: the k-vectors are all distinct, and none has all three indices zero.
All inputs are finite; a program needn't handle non-finite values.
Results may differ from the reference program's by a relative error of at most 0.0003.
Values sent between devices are 32-bit elements; how exact they have to be, the bound alone decides.
A program may use at most 64 MiB of HBM per device.

```python
import math
import jax
import jax.numpy as jnp
from jax import lax

KBLOCK = 4096
MMAX = 80
NCLS = 4
NSITES = 128
KVECS = 524288


def draw_miller(key, part):
    side = 2 * MMAX + 1
    cube = side * side * side
    centre = (cube - 1) // 2
    order = jax.random.permutation(jax.random.fold_in(key, 11), cube - 1).astype(jnp.int32)
    picked = order[:KVECS]
    picked = jnp.where(picked >= centre, picked + 1, picked)
    first = picked // (side * side) - MMAX
    second = picked // side % side - MMAX
    third = picked % side - MMAX
    return jnp.stack([first, second, third], axis=0).astype(jnp.int32)


def place_ends(values, rng, low, top_value):
    longest = values.shape.index(max(values.shape))
    spots = []
    for shift in (0, 1):
        where = [jax.random.randint(jax.random.fold_in(rng, axis), (), 0, length) for axis, length in enumerate(values.shape)]
        where[longest] = (where[longest] + shift) % values.shape[longest]
        spots.append(tuple(where))
    return values.at[spots[0]].set(low).at[spots[1]].set(top_value)


def level_of(rng, extent, cuts, smallest, top_value):
    loudness, own = 1.0, jax.random.fold_in(rng, 6)
    for axis_at, shards_of in cuts:
        steps = jnp.exp(jax.random.uniform(jax.random.fold_in(own, axis_at), (shards_of,), jnp.float32, smallest / len(cuts), top_value / len(cuts)))
        loudness = loudness * jnp.repeat(steps, extent[axis_at] // shards_of).reshape([-1 if axis == axis_at else 1 for axis in range(len(extent))])
    return loudness


def setup_inputs(seed: int = 0) -> dict:
    key_of = jax.random.split(jax.random.key(seed), 5)
    positions = jnp.clip(1.0 * jax.random.uniform(key_of[0], (3, NSITES), jnp.float32) ** level_of(key_of[0], (3, NSITES), ((1, 8),), -0.2, 0.2), 0.0, 1.0)
    site_class = place_ends(jax.random.randint(key_of[1], (NSITES,), 0, NCLS), jax.random.fold_in(key_of[1], 1), 0, NCLS - 1).astype(jnp.int32)
    class_charge = jnp.clip(jax.random.uniform(key_of[2], (NCLS,), jnp.float32, -2.0, 2.0), -2.0, 2.0)
    miller = draw_miller(jax.random.fold_in(key_of[4], 71), 0)
    return dict(positions=positions, site_class=site_class, class_charge=class_charge, miller=miller)


def charges_of(site_class, class_charge):
    onehot = (site_class[None, :] == jnp.arange(NCLS, dtype=jnp.int32)[:, None]).astype(jnp.float32)
    return jnp.dot(class_charge, onehot, precision=lax.Precision.HIGHEST)

def kernel_weights(mfloat):
    square = lax.optimization_barrier(jnp.sum(mfloat * mfloat, axis=0))
    limit = float(MMAX * MMAX)
    return limit * jnp.exp(-square / limit) / square

def phases(mblock, positions):
    angles = 2.0 * math.pi * (mblock[0][:, None] * positions[0][None, :] + mblock[1][:, None] * positions[1][None, :] + mblock[2][:, None] * positions[2][None, :])
    return (jnp.cos(angles), jnp.sin(angles))

def reference(positions, site_class, class_charge, miller):
    charge = charges_of(site_class, class_charge)
    mfloat = miller.astype(jnp.float32)
    weights = kernel_weights(mfloat)
    blocks = KVECS // KBLOCK
    mblocks = mfloat.reshape(3, blocks, KBLOCK).transpose(1, 0, 2)
    scale = 1.0 / math.sqrt(NSITES)

    def factor(mblock):
        cosine, sine = phases(mblock, positions)
        return (jnp.dot(cosine, charge, precision=lax.Precision.HIGHEST) * scale, jnp.dot(sine, charge, precision=lax.Precision.HIGHEST) * scale)
    creal, cimag = lax.map(factor, mblocks)
    wblocks = weights.reshape(blocks, KBLOCK)
    energy = jnp.sum(wblocks * (creal * creal + cimag * cimag)) / KVECS

    def accumulate(total, items):
        mblock, real_part, imag_part, wblock = items
        cosine, sine = phases(mblock, positions)
        grad_sine = mblock * (wblock * real_part)[None, :]
        grad_cosine = mblock * (wblock * imag_part)[None, :]
        total = total + jnp.dot(grad_sine, sine, precision=lax.Precision.HIGHEST) - jnp.dot(grad_cosine, cosine, precision=lax.Precision.HIGHEST)
        return (total, None)
    total, unused = lax.scan(accumulate, jnp.zeros((3, NSITES), jnp.float32), (mblocks, creal, cimag, wblocks))
    forces = 4.0 * math.pi / math.sqrt(NSITES * KVECS) * charge[None, :] * total
    return (forces, energy)
```

```python
import functools
import math

import jax
import jax.numpy as jnp
from jax import lax
from jax.experimental import pallas as pl
from jax.experimental.pallas import tpu as pltpu
from jax.sharding import PartitionSpec as P

MMAX = 80
NCLS = 4
MESH = pl.DeviceIdType.MESH
F32 = jnp.float32
BF16 = jnp.bfloat16
A0, A1, A2 = 1.5707884689227576, -0.645711988911062, 0.07766738858001387
TINY = 1e-24
KB = 512
ROWS = 16


def kernel(
    nsite, nka, nsites, kvecs,
    pos_ref, cls_ref, cc_ref, mil_ref,
    res_ref,
    mi, m16, wts, x16, alpha2, ca0, ca1, ca2, qabs, sh, ch, vbuf, facc, eacc, qtot, tbuf, gr1, gr2,
    ag_out, ag_in, rs_out, rs_in,
    mil_sem, ag_send, ag_recv, rs_send, rs_recv,
):
    ndev = nsite * nka
    si, ki = lax.axis_index("site"), lax.axis_index("ka")
    me = si * nka + ki
    ls = pos_ref.shape[1]
    sub = mi.shape[1]
    spd = nsites // ndev
    nblk = sub // KB

    mil_copy = pltpu.make_async_copy(
        mil_ref.at[:, pl.ds(pl.multiple_of(si * sub, 128), sub)], mi, mil_sem
    )
    mil_copy.start()

    cls = cls_ref[...]
    charge = jnp.zeros(cls.shape, F32)
    for c in range(NCLS):
        charge = jnp.where(cls == c, cc_ref[c], charge)
    ag_out[...] = jnp.zeros_like(ag_out)
    ag_out[0:3, 0:ls] = pos_ref[...]
    ag_out[3:4, 0:ls] = charge

    barrier = pltpu.get_barrier_semaphore()

    @pl.loop(1, ndev)
    def _(i):
        to = lax.rem(me + i, ndev)
        pl.semaphore_signal(
            barrier, inc=1, device_id=(lax.div(to, nka), lax.rem(to, nka)), device_id_type=MESH
        )

    mil_copy.wait()

    @pl.loop(0, nblk)
    def _(b):
        at = pl.ds(pl.multiple_of(b * KB, KB), KB)
        m = mi[:, at].astype(F32)
        sq = jnp.sum(m * m, axis=0, keepdims=True)
        limit = float(MMAX * MMAX)
        wts[:, at] = limit * jnp.exp(sq * (-1.0 / limit)) / sq
        m16[:, at] = jnp.concatenate(
            [m, m, m, jnp.ones((1, KB), F32), jnp.zeros((6, KB), F32)], axis=0
        ).astype(BF16)

    pl.semaphore_wait(barrier, ndev - 1)

    def ag_copy(src, to):
        return pltpu.make_async_remote_copy(
            src_ref=ag_out, dst_ref=ag_in.at[src], send_sem=ag_send.at[to],
            recv_sem=ag_recv.at[src], device_id=(to, ki), device_id_type=MESH,
        )

    @pl.loop(1, nsite)
    def _(i):
        ag_copy(si, lax.rem(si + i, nsite)).start()

    ag_in[si] = ag_out[...]

    @pl.loop(1, nsite)
    def _(i):
        other = lax.rem(si + i, nsite)
        ag_copy(other, other).wait_recv()

    per = 128 // ls
    for t in range(nsites // 128):
        allrows = ag_in[t * per]
        for i in range(1, per):
            allrows = allrows + pltpu.roll(ag_in[t * per + i], i * ls, 1)
        x = allrows[0:3]
        x = x - jnp.round(x)
        q = allrows[3:4]
        x1 = x.astype(BF16).astype(F32)
        x2 = (x - x1).astype(BF16).astype(F32)
        x3 = x - x1 - x2
        half = jnp.where(q < 0.0, 0.5, 0.0)
        qc = jnp.maximum(jnp.abs(q), TINY)
        al2 = jnp.sqrt(qc)
        al = jnp.sqrt(al2)
        rows = jnp.concatenate(
            [x1, x2, x3, half, al2, al * A0, al * A1, al * A2, jnp.abs(q), qc,
             jnp.zeros((112, 128), F32)], axis=0
        )
        cols = rows.T
        rs_ = pl.ds(t * 128, 128)
        x16[rs_, :] = cols[:, 0:16].astype(BF16)
        alpha2[rs_, :] = jnp.broadcast_to(cols[:, 10:11], (128, 128))
        ca0[rs_, :] = jnp.broadcast_to(cols[:, 11:12], (128, 128))
        ca1[rs_, :] = jnp.broadcast_to(cols[:, 12:13], (128, 128))
        ca2[rs_, :] = jnp.broadcast_to(cols[:, 13:14], (128, 128))
        qabs[rs_, 0:2] = cols[:, 14:16]
        total = jnp.broadcast_to(jnp.sum(qc, axis=1, keepdims=True), (1, 128))
        qtot[...] = total if t == 0 else qtot[...] + total

    facc[...] = jnp.zeros_like(facc)
    eacc[...] = jnp.zeros_like(eacc)
    isn = 1.0 / math.sqrt(nsites)

    def wide(v):
        return jnp.concatenate([v] * (KB // 128), axis=1)

    def cols_of(b):
        return pl.ds(pl.multiple_of(b * KB, KB), KB)

    def split(v, rows):
        hi = v.astype(BF16)
        vbuf[rows, 0:KB] = hi
        vbuf[rows, KB:] = (v - hi.astype(F32)).astype(BF16)

    def gather_forces(b):
        mb = m16[:, cols_of(b)]
        facc[...] += lax.dot_general(
            vbuf[...], jnp.concatenate([mb, mb], axis=1), (((1,), (1,)), ((), ())),
            preferred_element_type=F32,
        )

    def second(rr):
        split(sh[rr] * gr1[...] + ch[rr] * gr2[...], rr)

    extra = slice(nsites, nsites + ROWS)
    chunks = [slice(j * ROWS, (j + 1) * ROWS) for j in range(nsites // ROWS)]
    for buf in (sh, ch, gr1, gr2, vbuf):
        buf[...] = jnp.zeros_like(buf)
    tbuf[...] = jnp.dot(x16[...], m16[:, 0:KB], preferred_element_type=F32)

    @pl.loop(0, nblk)
    def _(b):
        gather_forces(jnp.maximum(b - 2, 0))
        turns = jnp.dot(
            x16[...], m16[:, cols_of(jnp.minimum(b + 1, nblk - 1))], preferred_element_type=F32
        )
        sums = sumc = None
        for j, rr in enumerate(chunks):
            second(rr)
            t = tbuf[rr]
            r = t - jnp.round(t)
            z = r * r
            s = r * (wide(ca0[rr]) + z * (wide(ca1[rr]) + z * wide(ca2[rr])))
            s2 = s * s
            u = wide(alpha2[rr]) - s2
            sc = s * (u * lax.rsqrt(u))
            dc = u - s2
            sj = sc * dc
            cj = sc * sc
            sh[rr] = sj
            ch[rr] = cj
            tbuf[rr] = turns[rr]
            sums = sj if j == 0 else sums + sj
            sumc = cj if j == 0 else sumc + cj
        split(jnp.broadcast_to(gr2[...], (ROWS, KB)), extra)
        cimag = (4.0 * isn) * jnp.sum(sums, axis=0, keepdims=True)
        creal = isn * (wide(qtot[...]) - 8.0 * jnp.sum(sumc, axis=0, keepdims=True))
        w = wts[:, cols_of(b)]
        g1 = w * creal
        g2 = w * cimag
        eacc[...] += g1 * creal + g2 * cimag
        gr1[...] = g1
        gr2[...] = 2.0 * g2

    gather_forces(max(nblk - 2, 0))
    for rr in chunks:
        second(rr)
    split(jnp.broadcast_to(gr2[...], (ROWS, KB)), extra)
    gather_forces(nblk - 1)

    energy = jnp.sum(eacc[...], axis=1, keepdims=True) * (1.0 / kvecs)
    fscale = 4.0 * math.pi / math.sqrt(nsites * kvecs)
    qa, qc = qabs[:, 0:1], qabs[:, 1:2]
    forces = (fscale * (qa / qc)) * (4.0 * facc[0:nsites] - (0.5 * qc) * facc[nsites : nsites + 1])
    lane = lax.broadcasted_iota(jnp.int32, forces.shape, 1)
    forces = jnp.where(lane == 3, energy, forces)
    rs_out[...] = jnp.zeros_like(rs_out)
    for p in range(ndev):
        rs_out[p, :, 0:16] = forces[p * spd : (p + 1) * spd]

    def rs_copy(src, to):
        return pltpu.make_async_remote_copy(
            src_ref=rs_out.at[to], dst_ref=rs_in.at[src], send_sem=rs_send.at[to],
            recv_sem=rs_recv.at[src], device_id=(lax.div(to, nka), lax.rem(to, nka)),
            device_id_type=MESH,
        )

    @pl.loop(1, ndev)
    def _(i):
        rs_copy(me, lax.rem(me + i, ndev)).start()

    rs_in[me] = rs_out[me]

    @pl.loop(1, ndev)
    def _(i):
        other = lax.rem(me + i, ndev)
        rs_copy(other, me).wait_recv()

    mine = jnp.sum(rs_in[...], axis=0)
    sub_i = lax.broadcasted_iota(jnp.int32, (spd, 128), 0)
    lane_i = lax.broadcasted_iota(jnp.int32, (spd, 128), 1)
    for d in range(3):
        row = jnp.sum(jnp.where(sub_i == lane_i, mine[:, d : d + 1], 0.0), axis=0, keepdims=True)
        res_ref[d : d + 1, :] = row
    res_ref[3:4, :] = jnp.broadcast_to(mine[0:1, 3:4], (1, 128))
    res_ref[4:8, :] = jnp.zeros((4, 128), F32)

    @pl.loop(1, ndev)
    def _(i):
        rs_copy(me, lax.rem(me + i, ndev)).wait_send()

    @pl.loop(1, nsite)
    def _(i):
        ag_copy(si, lax.rem(si + i, nsite)).wait_send()


def publish(res_ref, out_ref, en_ref):
    out_ref[...] = res_ref[0:3, 0 : out_ref.shape[1]]
    en_ref[...] = res_ref[3:4, 0:1]


def local(nsite, nka, positions, site_class, class_charge, miller):
    ndev = nsite * nka
    ls = positions.shape[1]
    nsites = ls * nsite
    kvecs = miller.shape[1] * nka
    sub = miller.shape[1] // nsite
    spd = nsites // ndev
    vmem = pl.BlockSpec(memory_space=pltpu.VMEM)
    summed = pl.pallas_call(
        functools.partial(kernel, nsite, nka, nsites, kvecs),
        out_shape=pltpu.VMEM((8, 128), F32),
        in_specs=[
            vmem, vmem, pl.BlockSpec(memory_space=pltpu.SMEM), pl.BlockSpec(memory_space=pl.ANY),
        ],
        out_specs=vmem,
        scratch_shapes=[
            pltpu.VMEM((3, sub), jnp.int32),
            pltpu.VMEM((16, sub), BF16),
            pltpu.VMEM((1, sub), F32),
            pltpu.VMEM((nsites, 16), BF16),
            pltpu.VMEM((nsites, 128), F32),
            pltpu.VMEM((nsites, 128), F32),
            pltpu.VMEM((nsites, 128), F32),
            pltpu.VMEM((nsites, 128), F32),
            pltpu.VMEM((nsites, 128), F32),
            pltpu.VMEM((nsites, KB), F32),
            pltpu.VMEM((nsites, KB), F32),
            pltpu.VMEM((nsites + ROWS, 2 * KB), BF16),
            pltpu.VMEM((nsites + ROWS, 16), F32),
            pltpu.VMEM((1, KB), F32),
            pltpu.VMEM((1, 128), F32),
            pltpu.VMEM((nsites, KB), F32),
            pltpu.VMEM((1, KB), F32),
            pltpu.VMEM((1, KB), F32),
            pltpu.VMEM((8, 128), F32),
            pltpu.VMEM((nsite, 8, 128), F32),
            pltpu.VMEM((ndev, spd, 128), F32),
            pltpu.VMEM((ndev, spd, 128), F32),
            pltpu.SemaphoreType.DMA,
            pltpu.SemaphoreType.DMA((nsite,)),
            pltpu.SemaphoreType.DMA((nsite,)),
            pltpu.SemaphoreType.DMA((ndev,)),
            pltpu.SemaphoreType.DMA((ndev,)),
        ],
        compiler_params=pltpu.CompilerParams(collective_id=0, has_side_effects=True),
        name="ewald",
    )(positions, site_class.reshape(1, ls), class_charge, miller)
    forces, energy = pl.pallas_call(
        publish,
        out_shape=(jax.ShapeDtypeStruct((3, spd), F32), jax.ShapeDtypeStruct((1, 1), F32)),
        in_specs=[vmem],
        out_specs=(vmem, vmem),
        name="publish",
    )(pltpu.with_memory_space_constraint(summed, pltpu.VMEM))
    return forces, energy[0, 0]


def solution(mesh):
    placed = (P(None, "site"), P("site"), P(), P(None, "ka"))
    return jax.shard_map(
        functools.partial(local, mesh.shape["site"], mesh.shape["ka"]),
        mesh=mesh,
        in_specs=placed,
        out_specs=(P(None, ("site", "ka")), P()),
        check_vma=False,
    )
```

```python
import functools
import math

import jax
import jax.numpy as jnp
from jax import lax
from jax.experimental import pallas as pl
from jax.experimental.pallas import tpu as pltpu
from jax.sharding import PartitionSpec as P

MMAX = 80
NCLS = 4
MESH = pl.DeviceIdType.MESH
F32 = jnp.float32
BF16 = jnp.bfloat16
A0, A1, A2 = 1.5707884689227576, -0.645711988911062, 0.07766738858001387
TINY = 1e-24
UNITS = 4
SKEW = (1, 0)
KBW = 1024


def shares(nsite, units):
    total, top = SKEW[0] * nsite, SKEW[1]
    span = nsite * (total - top * nsite)

    def first(s):
        return units * s * (total - top * s) // span

    return first, max(first(s + 1) - first(s) for s in range(nsite))


def kernel(
    nsite, nka, nsites, kvecs, kb,
    pos_ref, cls_ref, cc_ref, mil_ref,
    res_ref,
    posv, clsv, ccv, mi, m16, wts, pbuf, xs, co, tbuf, psin, pcos, ssin, scos,
    qrow, qtot, g1v, g2v, facc, eacc,
    ag_out, ag_in, rs_out, rs_in,
    pos_sem, cls_sem, cc_sem, mil_sem, ag_send, ag_recv, rs_send, rs_recv, ready, kin, kall,
):
    ndev = nsite * nka
    si, ki = lax.axis_index("site"), lax.axis_index("ka")
    me = si * nka + ki
    ls = posv.shape[1]
    spd = nsites // ndev
    units = mil_ref.shape[1] // kb
    first, most = shares(nsite, units)
    low = first(si)
    n = first(si + 1) - low
    base = jnp.minimum(low, units - most)
    shift = low - base

    pos_copy = pltpu.make_async_copy(pos_ref, posv, pos_sem)
    cls_copy = pltpu.make_async_copy(cls_ref, clsv, cls_sem)
    cc_copy = pltpu.make_async_copy(cc_ref, ccv, cc_sem)
    mil_copy = pltpu.make_async_copy(
        mil_ref.at[:, pl.ds(pl.multiple_of(base * kb, 128), most * kb)], mi, mil_sem
    )
    pos_copy.start()
    cls_copy.start()
    cc_copy.start()
    mil_copy.start()

    barrier = pltpu.get_barrier_semaphore()

    def tell(sem, s, k):
        pl.semaphore_signal(sem, inc=1, device_id=(s, k), device_id_type=MESH)

    @pl.loop(si + 1, nsite)
    def _(s):
        tell(barrier, s, ki)

    @pl.loop(ki + 1, nka)
    def _(k):
        tell(barrier, si, k)

    ssin[...] = jnp.zeros_like(ssin)
    scos[...] = jnp.zeros_like(scos)
    qrow[...] = jnp.zeros_like(qrow)
    qtot[...] = jnp.zeros_like(qtot)
    facc[...] = jnp.zeros_like(facc)
    eacc[...] = jnp.zeros_like(eacc)
    pbuf[...] = jnp.zeros_like(pbuf)

    pos_copy.wait()
    cls_copy.wait()
    cc_copy.wait()
    cls = clsv[...]
    charge = jnp.zeros(cls.shape, F32)
    for c in range(NCLS):
        charge = jnp.where(cls == c, jnp.broadcast_to(ccv[0:1, c : c + 1], cls.shape), charge)
    pbuf[0:3, 0:ls] = posv[...]
    pbuf[3:4, 0:ls] = charge
    x = pbuf[0:3]
    x = x - jnp.round(x)
    q = pbuf[3:4]
    x1 = x.astype(BF16).astype(F32)
    x2 = (x - x1).astype(BF16).astype(F32)
    x3 = x - x1 - x2
    half = jnp.where(q < 0.0, 0.5, 0.0)
    qc = jnp.maximum(jnp.abs(q), TINY)
    al2 = jnp.sqrt(qc)
    al = jnp.sqrt(al2)
    rows = jnp.concatenate(
        [x1, x2, x3, half, jnp.zeros((6, 128), F32), al2, al * A0, al * A1, al * A2,
         jnp.zeros((108, 128), F32)], axis=0
    )
    cols = rows.T
    own = lax.broadcasted_iota(jnp.int32, (1, 128), 1) < ls
    qown = jnp.where(own, qc, 0.0)
    tail = jnp.concatenate(
        [qown, jnp.where(own, jnp.abs(q) / qc, 0.0),
         jnp.broadcast_to(jnp.sum(qown, axis=1, keepdims=True), (1, 128)),
         jnp.zeros((5, 128), F32)], axis=0
    )
    ag_out[0:ls] = cols[0:ls]
    ag_out[ls:] = tail
    ag_in[si] = ag_out[...]

    @pl.when(si + ki > 0)
    def _():
        pl.semaphore_wait(barrier, si + ki)

    def ag_copy(src, to):
        return pltpu.make_async_remote_copy(
            src_ref=ag_out, dst_ref=ag_in.at[src], send_sem=ag_send.at[to],
            recv_sem=ag_recv.at[src], device_id=(to, ki), device_id_type=MESH,
        )

    @pl.loop(0, si)
    def _(s):
        tell(ready.at[si], s, ki)
        ag_copy(si, s).start()

    @pl.loop(0, ki)
    def _(k):
        tell(kin, si, k)

    mil_copy.wait()

    @pl.loop(0, n * (kb // KBW))
    def _(b):
        at = pl.ds(pl.multiple_of(b * KBW, KBW), KBW)
        m = mi[:, pl.ds(pl.multiple_of(shift * kb + b * KBW, KBW), KBW)].astype(F32)
        sq = jnp.sum(m * m, axis=0, keepdims=True)
        limit = float(MMAX * MMAX)
        wts[:, at] = limit * jnp.exp(sq * (-1.0 / limit)) / sq
        m16[:, at] = jnp.concatenate(
            [m, m, m, jnp.ones((1, KBW), F32), jnp.zeros((6, KBW), F32)], axis=0
        ).astype(BF16)

    def source(i):
        if nsite & (nsite - 1):
            return lax.rem(si + i, nsite)
        out, bit = 0, 1
        while bit < nsite:
            out = out + bit * lax.rem(lax.div(si, bit) + lax.div(i, bit), 2)
            bit *= 2
        return out

    def prepare(i):
        src = source(i)
        slot = lax.rem(i, 2)
        xs[slot] = ag_in[src, 0:ls, 0:16].astype(BF16)
        for c in range(4):
            co[slot, c] = jnp.broadcast_to(ag_in[src, 0:ls, 16 + c : 17 + c], (ls, 128))
        both = ag_in[src, ls : ls + 8]
        if nsites > 128:
            both = jnp.concatenate([both, jnp.zeros((8, nsites - 128), F32)], axis=1)
        qrow[...] += pltpu.roll(both, src * ls, 1)
        qtot[...] += ag_in[src, ls + 2 : ls + 3]

    def block_of(b):
        return pl.ds(pl.multiple_of(b * kb, kb), kb)

    prepare(0)
    tbuf[...] = jnp.dot(xs[0], m16[:, 0:kb], preferred_element_type=F32)

    @pl.loop(0, nsite)
    def _(i):
        src = source(i)
        slot = lax.rem(i, 2)

        @pl.loop(0, n)
        def _(b):
            last = lax.div(b + 1, n)

            @pl.when((last == 1) & (i < nsite - 1))
            def _():
                to = si + i + 2 - lax.div(1, i + 1)
                for o in range(2):
                    @pl.when((lax.rem(i, 2) + lax.div(1, i + 1) > 0) & (to + o < nsite))
                    def _():
                        pl.semaphore_wait(ready.at[to + o], 1)
                        ag_copy(si, to + o).start()

                nxt = source(i + 1)
                ag_copy(nxt, nxt).wait_recv()
                prepare(i + 1)

            turns = jnp.dot(
                xs[lax.rem(i + last, 2)], m16[:, block_of(b + 1 - last * n)],
                preferred_element_type=F32,
            )
            c0, c1, c2, c3 = co[slot, 0], co[slot, 1], co[slot, 2], co[slot, 3]
            for l in range(kb // 128):
                ln = slice(l * 128, (l + 1) * 128)
                at = pl.ds(pl.multiple_of(b * kb + l * 128, 128), 128)
                t = tbuf[:, ln]
                r = t - jnp.round(t)
                z = r * r
                s = r * (c1 + z * (c2 + z * c3))
                s2 = s * s
                u = c0 - s2
                sc = s * (u * lax.rsqrt(u))
                dc = u - s2
                sj = sc * dc
                cj = sc * sc
                psin[src, :, at] = sj
                pcos[src, :, at] = cj
                tbuf[:, ln] = turns[:, ln]
                sums, sumc = sj[0:8], cj[0:8]
                for g in range(1, ls // 8):
                    sums = sums + sj[8 * g : 8 * g + 8]
                    sumc = sumc + cj[8 * g : 8 * g + 8]
                ssin[:, at] += sums
                scos[:, at] += sumc

    @pl.when(ki < nka - 1)
    def _():
        pl.semaphore_wait(kin, nka - 1 - ki)

    @pl.loop(1, nka)
    def _(i):
        tell(kall, si, lax.rem(ki + i, nka))

    isn = 1.0 / math.sqrt(nsites)
    steps = n

    def step_of(j):
        return pl.ds(pl.multiple_of(j * kb, kb), kb)

    def weigh(j, counts):
        at = step_of(j)
        cimag = (4.0 * isn) * jnp.sum(ssin[:, at], axis=0, keepdims=True)
        total = jnp.concatenate([qtot[...]] * (kb // 128), axis=1)
        creal = isn * (total - 8.0 * jnp.sum(scos[:, at], axis=0, keepdims=True))
        w = wts[:, at]
        g1 = w * creal
        g2 = w * cimag
        e = g1 * creal + g2 * cimag
        eacc[...] += e if counts is None else jnp.where(counts, e, 0.0)
        g1v[...] = g1
        g2v[...] = 2.0 * g2

    weigh(0, None)

    @pl.loop(0, steps)
    def _(j):
        at = step_of(j)
        v = (psin[:, :, at] * g1v[...] + pcos[:, :, at] * g2v[...]).reshape(nsites, kb)
        hi = v.astype(BF16)
        lo = (v - hi.astype(F32)).astype(BF16)
        m = m16[:, at]
        dims = (((1,), (1,)), ((), ()))
        facc[...] += lax.dot_general(m, hi, dims, preferred_element_type=F32) + lax.dot_general(
            m, lo, dims, preferred_element_type=F32
        )
        weigh(jnp.minimum(j + 1, steps - 1), j + 1 < steps)

    en = eacc[:, 0:128]
    for l in range(1, kb // 128):
        en = en + eacc[:, l * 128 : (l + 1) * 128]
    if nsites > 128:
        en = jnp.concatenate([en, jnp.zeros((1, nsites - 128), F32)], axis=1)
    rs_out[...] = jnp.concatenate([facc[0:3], en], axis=0)

    pl.semaphore_wait(kall, nka - 1)

    def rs_copy(to):
        return pltpu.make_async_remote_copy(
            src_ref=rs_out, dst_ref=rs_in.at[me], send_sem=rs_send, recv_sem=rs_recv,
            device_id=(lax.div(to, nka), lax.rem(to, nka)), device_id_type=MESH,
        )

    @pl.loop(0, ndev)
    def _(to):
        @pl.when(to != me)
        def _():
            rs_copy(to).start()

    rs_in[me] = rs_out[...]
    others = rs_in.at[pl.ds(0, ndev - 1)]
    pltpu.make_async_copy(others, others, rs_recv).wait()

    total = jnp.sum(rs_in[...], axis=0)
    fall = total[0:3]
    qall, ratio = qrow[0:1], qrow[1:2]
    fscale = 16.0 * math.pi / math.sqrt(nsites * kvecs)
    mean = jnp.sum(fall, axis=1, keepdims=True) / jnp.sum(qall, axis=1, keepdims=True)
    forces = (fscale * ratio) * (fall - qall * mean)
    energy = jnp.sum(total[3:4], axis=1, keepdims=True) * (1.0 / kvecs)
    mine = pltpu.roll(
        jnp.concatenate([forces, jnp.zeros((5, nsites), F32)], axis=0), nsites - me * spd, 1
    )
    res_ref[...] = mine[:, 0:128]
    res_ref[3:4, :] = jnp.broadcast_to(energy, (1, 128))

    pltpu.make_async_copy(others, others, rs_send).wait()

    @pl.loop(1, nsite)
    def _(i):
        ag_copy(si, lax.rem(si + i, nsite)).wait_send()


def publish(res_ref, out_ref, en_ref):
    out_ref[...] = res_ref[0:3, 0 : out_ref.shape[1]]
    en_ref[...] = res_ref[3:4, 0:1]


def local(nsite, nka, positions, site_class, class_charge, miller):
    ndev = nsite * nka
    ls = positions.shape[1]
    nsites = ls * nsite
    kvecs = miller.shape[1] * nka
    spd = nsites // ndev
    kb = miller.shape[1] // (nsite * UNITS)
    span = shares(nsite, miller.shape[1] // kb)[1] * kb
    vmem = pl.BlockSpec(memory_space=pltpu.VMEM)
    summed = pl.pallas_call(
        functools.partial(kernel, nsite, nka, nsites, kvecs, kb),
        out_shape=pltpu.VMEM((8, 128), F32),
        in_specs=[pl.BlockSpec(memory_space=pl.ANY)] * 4,
        out_specs=vmem,
        scratch_shapes=[
            pltpu.VMEM((3, ls), F32),
            pltpu.VMEM((1, ls), jnp.int32),
            pltpu.VMEM((1, NCLS), F32),
            pltpu.VMEM((3, span), jnp.int32),
            pltpu.VMEM((16, span), BF16),
            pltpu.VMEM((1, span), F32),
            pltpu.VMEM((8, 128), F32),
            pltpu.VMEM((2, ls, 16), BF16),
            pltpu.VMEM((2, 4, ls, 128), F32),
            pltpu.VMEM((ls, kb), F32),
            pltpu.VMEM((nsite, ls, span), F32),
            pltpu.VMEM((nsite, ls, span), F32),
            pltpu.VMEM((8, span), F32),
            pltpu.VMEM((8, span), F32),
            pltpu.VMEM((8, nsites), F32),
            pltpu.VMEM((1, 128), F32),
            pltpu.VMEM((1, kb), F32),
            pltpu.VMEM((1, kb), F32),
            pltpu.VMEM((16, nsites), F32),
            pltpu.VMEM((1, kb), F32),
            pltpu.VMEM((ls + 8, 128), F32),
            pltpu.VMEM((nsite, ls + 8, 128), F32),
            pltpu.VMEM((4, nsites), F32),
            pltpu.VMEM((ndev, 4, nsites), F32),
            pltpu.SemaphoreType.DMA,
            pltpu.SemaphoreType.DMA,
            pltpu.SemaphoreType.DMA,
            pltpu.SemaphoreType.DMA,
            pltpu.SemaphoreType.DMA((nsite,)),
            pltpu.SemaphoreType.DMA((nsite,)),
            pltpu.SemaphoreType.DMA,
            pltpu.SemaphoreType.DMA,
            pltpu.SemaphoreType.REGULAR((nsite,)),
            pltpu.SemaphoreType.REGULAR,
            pltpu.SemaphoreType.REGULAR,
        ],
        compiler_params=pltpu.CompilerParams(collective_id=0, has_side_effects=True),
        name="ewald",
    )(positions, site_class.reshape(1, ls), class_charge.reshape(1, NCLS), miller)
    forces, energy = pl.pallas_call(
        publish,
        out_shape=(jax.ShapeDtypeStruct((3, spd), F32), jax.ShapeDtypeStruct((1, 1), F32)),
        in_specs=[vmem],
        out_specs=(vmem, vmem),
        name="publish",
    )(pltpu.with_memory_space_constraint(summed, pltpu.VMEM))
    return forces, energy[0, 0]


def solution(mesh):
    placed = (P(None, "site"), P("site"), P(), P(None, "ka"))
    return jax.shard_map(
        functools.partial(local, mesh.shape["site"], mesh.shape["ka"]),
        mesh=mesh,
        in_specs=placed,
        out_specs=(P(None, ("site", "ka")), P()),
        check_vma=False,
    )
```

```python
import functools
import math

import jax
import jax.numpy as jnp
from jax import lax
from jax.experimental import pallas as pl
from jax.experimental.pallas import tpu as pltpu
from jax.sharding import PartitionSpec as P

MMAX = 80
NCLS = 4
MESH = pl.DeviceIdType.MESH
F32 = jnp.float32
BF16 = jnp.bfloat16
A0, A1, A2 = 1.5707884689227576, -0.645711988911062, 0.07766738858001387
TINY = 1e-24
UNITS = 4
SKEW = (28, 8)
OFFER = (2, 2)
KBW = 1024


def shares(nsite, units):
    total, top = SKEW[0] * nsite, SKEW[1]
    span = nsite * (total - top * nsite)

    def first(s):
        return units * s * (total - top * s) // span

    sizes = [first(s + 1) - first(s) for s in range(nsite)]
    return first, max(sizes), min(sizes)


def kernel(
    nsite, nka, nsites, kvecs, kb,
    pos_ref, cls_ref, cc_ref, mil_ref,
    res_ref,
    posv, clsv, ccv, mi, m16, wts, pbuf, xs, co, tbuf, psin, pcos, ssin, scos,
    qrow, qtot, g1v, g2v, facc, eacc,
    ag_out, ag_in, rs_out, rs_in,
    pos_sem, cls_sem, cc_sem, mil_sem, ag_send, ag_recv, rs_send, rs_recv, ready, kin, kall,
):
    ndev = nsite * nka
    si, ki = lax.axis_index("site"), lax.axis_index("ka")
    me = si * nka + ki
    ls = posv.shape[1]
    spd = nsites // ndev
    units = mil_ref.shape[1] // kb
    first, most, least = shares(nsite, units)
    offers = [min(OFFER[0] + OFFER[1] * p, nsite * least - 1) for p in range(nsite // 2)]
    low = first(si)
    n = first(si + 1) - low
    base = jnp.minimum(low, units - most)
    shift = low - base

    pos_copy = pltpu.make_async_copy(pos_ref, posv, pos_sem)
    cls_copy = pltpu.make_async_copy(cls_ref, clsv, cls_sem)
    cc_copy = pltpu.make_async_copy(cc_ref, ccv, cc_sem)
    mil_copy = pltpu.make_async_copy(
        mil_ref.at[:, pl.ds(pl.multiple_of(base * kb, 128), most * kb)], mi, mil_sem
    )
    pos_copy.start()
    cls_copy.start()
    cc_copy.start()
    mil_copy.start()

    barrier = pltpu.get_barrier_semaphore()

    def tell(sem, s, k):
        pl.semaphore_signal(sem, inc=1, device_id=(s, k), device_id_type=MESH)

    @pl.loop(si + 1, nsite)
    def _(s):
        tell(barrier, s, ki)

    @pl.loop(ki + 1, nka)
    def _(k):
        tell(barrier, si, k)

    pbuf[...] = jnp.zeros_like(pbuf)

    pos_copy.wait()
    cls_copy.wait()
    cc_copy.wait()
    cls = clsv[...]
    charge = jnp.zeros(cls.shape, F32)
    for c in range(NCLS):
        charge = jnp.where(cls == c, jnp.broadcast_to(ccv[0:1, c : c + 1], cls.shape), charge)
    pbuf[0:3, 0:ls] = posv[...]
    pbuf[3:4, 0:ls] = charge
    x = pbuf[0:3]
    x = x - jnp.round(x)
    q = pbuf[3:4]
    x1 = x.astype(BF16).astype(F32)
    x2 = (x - x1).astype(BF16).astype(F32)
    x3 = x - x1 - x2
    half = jnp.where(q < 0.0, 0.5, 0.0)
    qc = jnp.maximum(jnp.abs(q), TINY)
    al2 = jnp.sqrt(qc)
    al = jnp.sqrt(al2)
    rows = jnp.concatenate(
        [x1, x2, x3, half, jnp.zeros((6, 128), F32), al2, al * A0, al * A1, al * A2,
         jnp.zeros((108, 128), F32)], axis=0
    )
    cols = rows.T
    own = lax.broadcasted_iota(jnp.int32, (1, 128), 1) < ls
    qown = jnp.where(own, qc, 0.0)
    tail = jnp.concatenate(
        [qown, jnp.where(own, jnp.abs(q) / qc, 0.0),
         jnp.broadcast_to(jnp.sum(qown, axis=1, keepdims=True), (1, 128)),
         jnp.zeros((5, 128), F32)], axis=0
    )
    ag_out[0:ls] = cols[0:ls]
    ag_out[ls:] = tail
    ag_in[si] = ag_out[...]

    @pl.when(si + ki > 0)
    def _():
        pl.semaphore_wait(barrier, si + ki)

    def ag_copy(src, to):
        return pltpu.make_async_remote_copy(
            src_ref=ag_out, dst_ref=ag_in.at[src], send_sem=ag_send.at[to],
            recv_sem=ag_recv.at[src], device_id=(to, ki), device_id_type=MESH,
        )

    @pl.loop(0, si)
    def _(s):
        tell(ready.at[si], s, ki)
        ag_copy(si, s).start()

    @pl.loop(0, ki)
    def _(k):
        tell(kin, si, k)

    ssin[...] = jnp.zeros_like(ssin)
    scos[...] = jnp.zeros_like(scos)
    qrow[...] = jnp.zeros_like(qrow)
    qtot[...] = jnp.zeros_like(qtot)
    facc[...] = jnp.zeros_like(facc)
    eacc[...] = jnp.zeros_like(eacc)
    mil_copy.wait()

    @pl.loop(0, n * (kb // KBW))
    def _(b):
        at = pl.ds(pl.multiple_of(b * KBW, KBW), KBW)
        m = mi[:, pl.ds(pl.multiple_of(shift * kb + b * KBW, KBW), KBW)].astype(F32)
        sq = jnp.sum(m * m, axis=0, keepdims=True)
        limit = float(MMAX * MMAX)
        wts[:, at] = limit * jnp.exp(sq * (-1.0 / limit)) / sq
        m16[:, at] = jnp.concatenate(
            [m, m, m, jnp.ones((1, KBW), F32), jnp.zeros((6, KBW), F32)], axis=0
        ).astype(BF16)

    def source(i):
        if nsite & (nsite - 1):
            return lax.rem(si + i, nsite)
        out, bit = 0, 1
        while bit < nsite:
            out = out + bit * lax.rem(lax.div(si, bit) + lax.div(i, bit), 2)
            bit *= 2
        return out

    def prepare(i):
        src = source(i)
        slot = lax.rem(i, 2)
        xs[slot] = ag_in[src, 0:ls, 0:16].astype(BF16)
        for c in range(4):
            co[slot, c] = jnp.broadcast_to(ag_in[src, 0:ls, 16 + c : 17 + c], (ls, 128))
        both = ag_in[src, ls : ls + 8]
        if nsites > 128:
            both = jnp.concatenate([both, jnp.zeros((8, nsites - 128), F32)], axis=1)
        qrow[...] += pltpu.roll(both, src * ls, 1)
        qtot[...] += ag_in[src, ls + 2 : ls + 3]

    def block_of(b):
        return pl.ds(pl.multiple_of(b * kb, kb), kb)

    prepare(0)
    tbuf[...] = jnp.dot(xs[0], m16[:, 0:kb], preferred_element_type=F32)

    def turn(i, b, slot, at_next):
        src = source(i)
        mine = lax.rem(i, 2)
        turns = jnp.dot(xs[slot], m16[:, at_next], preferred_element_type=F32)
        c0, c1, c2, c3 = co[mine, 0], co[mine, 1], co[mine, 2], co[mine, 3]
        for l in range(kb // 128):
            ln = slice(l * 128, (l + 1) * 128)
            at = pl.ds(pl.multiple_of(b * kb + l * 128, 128), 128)
            t = tbuf[:, ln]
            r = t - jnp.round(t)
            z = r * r
            s = r * (c1 + z * (c2 + z * c3))
            s2 = s * s
            u = c0 - s2
            sc = s * (u * lax.rsqrt(u))
            dc = u - s2
            sj = sc * dc
            cj = sc * sc
            psin[src, :, at] = sj
            pcos[src, :, at] = cj
            tbuf[:, ln] = turns[:, ln]
            sums, sumc = sj[0:8], cj[0:8]
            for g in range(1, ls // 8):
                sums = sums + sj[8 * g : 8 * g + 8]
                sumc = sumc + cj[8 * g : 8 * g + 8]
            ssin[:, at] += sums
            scos[:, at] += sumc

    def offer(g):
        for p, when in enumerate(offers):
            @pl.when(g == when)
            def _():
                for o in (2 * p + 1, 2 * p + 2):
                    @pl.when(si + o < nsite)
                    def _():
                        pl.semaphore_wait(ready.at[si + o], 1)
                        ag_copy(si, si + o).start()

    @pl.loop(0, nsite)
    def _(i):
        @pl.loop(0, n - 1)
        def _(b):
            offer(i * n + b)
            turn(i, b, lax.rem(i, 2), block_of(b + 1))

        offer(i * n + n - 1)

        @pl.when(i < nsite - 1)
        def _():
            nxt = source(i + 1)
            ag_copy(nxt, nxt).wait_recv()
            prepare(i + 1)

        turn(i, n - 1, lax.rem(i + 1, 2), block_of(0))

    @pl.when(ki < nka - 1)
    def _():
        pl.semaphore_wait(kin, nka - 1 - ki)

    @pl.loop(1, nka)
    def _(i):
        tell(kall, si, lax.rem(ki + i, nka))

    isn = 1.0 / math.sqrt(nsites)
    steps = n

    def step_of(j):
        return pl.ds(pl.multiple_of(j * kb, kb), kb)

    def weigh(j, counts):
        at = step_of(j)
        cimag = (4.0 * isn) * jnp.sum(ssin[:, at], axis=0, keepdims=True)
        total = jnp.concatenate([qtot[...]] * (kb // 128), axis=1)
        creal = isn * (total - 8.0 * jnp.sum(scos[:, at], axis=0, keepdims=True))
        w = wts[:, at]
        g1 = w * creal
        g2 = w * cimag
        e = g1 * creal + g2 * cimag
        eacc[...] += e if counts is None else jnp.where(counts, e, 0.0)
        g1v[...] = g1
        g2v[...] = 2.0 * g2

    weigh(0, None)

    @pl.loop(0, steps)
    def _(j):
        at = step_of(j)
        v = (psin[:, :, at] * g1v[...] + pcos[:, :, at] * g2v[...]).reshape(nsites, kb)
        hi = v.astype(BF16)
        lo = (v - hi.astype(F32)).astype(BF16)
        m = m16[:, at]
        dims = (((1,), (1,)), ((), ()))
        both = lax.dot_general(
            m, jnp.concatenate([hi, lo], axis=0), dims, preferred_element_type=F32
        )
        facc[...] += both[:, 0:nsites] + both[:, nsites:]
        weigh(jnp.minimum(j + 1, steps - 1), j + 1 < steps)

    en = eacc[:, 0:128]
    for l in range(1, kb // 128):
        en = en + eacc[:, l * 128 : (l + 1) * 128]
    if nsites > 128:
        en = jnp.concatenate([en, jnp.zeros((1, nsites - 128), F32)], axis=1)
    rs_out[...] = jnp.concatenate([facc[0:3], en], axis=0)

    pl.semaphore_wait(kall, nka - 1)

    def rs_copy(to):
        return pltpu.make_async_remote_copy(
            src_ref=rs_out, dst_ref=rs_in.at[me], send_sem=rs_send, recv_sem=rs_recv,
            device_id=(lax.div(to, nka), lax.rem(to, nka)), device_id_type=MESH,
        )

    @pl.loop(0, ndev)
    def _(to):
        @pl.when(to != me)
        def _():
            rs_copy(to).start()

    rs_in[me] = rs_out[...]
    others = rs_in.at[pl.ds(0, ndev - 1)]
    pltpu.make_async_copy(others, others, rs_recv).wait()

    total = jnp.sum(rs_in[...], axis=0)
    fall = total[0:3]
    qall, ratio = qrow[0:1], qrow[1:2]
    fscale = 16.0 * math.pi / math.sqrt(nsites * kvecs)
    mean = jnp.sum(fall, axis=1, keepdims=True) / jnp.sum(qall, axis=1, keepdims=True)
    forces = (fscale * ratio) * (fall - qall * mean)
    energy = jnp.sum(total[3:4], axis=1, keepdims=True) * (1.0 / kvecs)
    mine = pltpu.roll(
        jnp.concatenate([forces, jnp.zeros((5, nsites), F32)], axis=0), nsites - me * spd, 1
    )
    res_ref[...] = mine[:, 0:128]
    res_ref[3:4, :] = jnp.broadcast_to(energy, (1, 128))

    pltpu.make_async_copy(others, others, rs_send).wait()

    @pl.loop(1, nsite)
    def _(i):
        ag_copy(si, lax.rem(si + i, nsite)).wait_send()


def publish(res_ref, out_ref, en_ref):
    out_ref[...] = res_ref[0:3, 0 : out_ref.shape[1]]
    en_ref[...] = res_ref[3:4, 0:1]


def local(nsite, nka, positions, site_class, class_charge, miller):
    ndev = nsite * nka
    ls = positions.shape[1]
    nsites = ls * nsite
    kvecs = miller.shape[1] * nka
    spd = nsites // ndev
    kb = miller.shape[1] // (nsite * UNITS)
    span = shares(nsite, miller.shape[1] // kb)[1] * kb
    vmem = pl.BlockSpec(memory_space=pltpu.VMEM)
    summed = pl.pallas_call(
        functools.partial(kernel, nsite, nka, nsites, kvecs, kb),
        out_shape=pltpu.VMEM((8, 128), F32),
        in_specs=[pl.BlockSpec(memory_space=pl.ANY)] * 4,
        out_specs=vmem,
        scratch_shapes=[
            pltpu.VMEM((3, ls), F32),
            pltpu.VMEM((1, ls), jnp.int32),
            pltpu.VMEM((1, NCLS), F32),
            pltpu.VMEM((3, span), jnp.int32),
            pltpu.VMEM((16, span), BF16),
            pltpu.VMEM((1, span), F32),
            pltpu.VMEM((8, 128), F32),
            pltpu.VMEM((2, ls, 16), BF16),
            pltpu.VMEM((2, 4, ls, 128), F32),
            pltpu.VMEM((ls, kb), F32),
            pltpu.VMEM((nsite, ls, span), F32),
            pltpu.VMEM((nsite, ls, span), F32),
            pltpu.VMEM((8, span), F32),
            pltpu.VMEM((8, span), F32),
            pltpu.VMEM((8, nsites), F32),
            pltpu.VMEM((1, 128), F32),
            pltpu.VMEM((1, kb), F32),
            pltpu.VMEM((1, kb), F32),
            pltpu.VMEM((16, nsites), F32),
            pltpu.VMEM((1, kb), F32),
            pltpu.VMEM((ls + 8, 128), F32),
            pltpu.VMEM((nsite, ls + 8, 128), F32),
            pltpu.VMEM((4, nsites), F32),
            pltpu.VMEM((ndev, 4, nsites), F32),
            pltpu.SemaphoreType.DMA,
            pltpu.SemaphoreType.DMA,
            pltpu.SemaphoreType.DMA,
            pltpu.SemaphoreType.DMA,
            pltpu.SemaphoreType.DMA((nsite,)),
            pltpu.SemaphoreType.DMA((nsite,)),
            pltpu.SemaphoreType.DMA,
            pltpu.SemaphoreType.DMA,
            pltpu.SemaphoreType.REGULAR((nsite,)),
            pltpu.SemaphoreType.REGULAR,
            pltpu.SemaphoreType.REGULAR,
        ],
        compiler_params=pltpu.CompilerParams(collective_id=0, has_side_effects=True),
        name="ewald",
    )(positions, site_class.reshape(1, ls), class_charge.reshape(1, NCLS), miller)
    forces, energy = pl.pallas_call(
        publish,
        out_shape=(jax.ShapeDtypeStruct((3, spd), F32), jax.ShapeDtypeStruct((1, 1), F32)),
        in_specs=[vmem],
        out_specs=(vmem, vmem),
        name="publish",
    )(pltpu.with_memory_space_constraint(summed, pltpu.VMEM))
    return forces, energy[0, 0]


def solution(mesh):
    placed = (P(None, "site"), P("site"), P(), P(None, "ka"))
    return jax.shard_map(
        functools.partial(local, mesh.shape["site"], mesh.shape["ka"]),
        mesh=mesh,
        in_specs=placed,
        out_specs=(P(None, ("site", "ka")), P()),
        check_vma=False,
    )
```

```python
import functools
import math

import jax
import jax.numpy as jnp
from jax import lax
from jax.experimental import pallas as pl
from jax.experimental.pallas import tpu as pltpu
from jax.sharding import PartitionSpec as P

MMAX = 80
NCLS = 4
MESH = pl.DeviceIdType.MESH
F32 = jnp.float32
BF16 = jnp.bfloat16
A0, A1, A2 = 1.5707884689227576, -0.645711988911062, 0.07766738858001387
TINY = 1e-24
UNITS = 4
SKEW = (36, 8)
OFFER = (1, 3)
WIDE = 4096


def shares(nsite, units):
    total, top = SKEW[0] * nsite, SKEW[1]
    span = nsite * (total - top * nsite)

    def first(s):
        return units * s * (total - top * s) // span

    sizes = [first(s + 1) - first(s) for s in range(nsite)]
    return first, max(sizes), min(sizes)


def kernel(
    nsite, nka, nsites, kvecs, kb,
    pos_ref, cls_ref, cc_ref, mil_ref,
    res_ref,
    posv, clsv, ccv, mi, m16, wts, pbuf, xs, co, tbuf, psin, pcos, ssin, scos,
    qrow, qtot, g1v, g2v, facc, eacc,
    ag_out, ag_in, rs_out, rs_in,
    pos_sem, cls_sem, cc_sem, mil_sem, ag_send, ag_recv, rs_send, rs_recv, ready, kin, kall,
):
    ndev = nsite * nka
    si, ki = lax.axis_index("site"), lax.axis_index("ka")
    me = si * nka + ki
    ls = posv.shape[1]
    spd = nsites // ndev
    units = mil_ref.shape[1] // kb
    first, most, least = shares(nsite, units)
    offers = [min(OFFER[0] + OFFER[1] * p, nsite * least - 1) for p in range(nsite // 2)]
    low = first(si)
    n = first(si + 1) - low
    base = jnp.minimum(low, units - most)
    shift = low - base

    pos_copy = pltpu.make_async_copy(pos_ref, posv, pos_sem)
    cls_copy = pltpu.make_async_copy(cls_ref, clsv, cls_sem)
    cc_copy = pltpu.make_async_copy(cc_ref, ccv, cc_sem)
    mil_copy = pltpu.make_async_copy(
        mil_ref.at[:, pl.ds(pl.multiple_of(base * kb, 128), most * kb)], mi, mil_sem
    )
    pos_copy.start()
    cls_copy.start()
    cc_copy.start()
    mil_copy.start()

    barrier = pltpu.get_barrier_semaphore()

    def tell(sem, s, k):
        pl.semaphore_signal(sem, inc=1, device_id=(s, k), device_id_type=MESH)

    @pl.loop(si + 1, nsite)
    def _(s):
        tell(barrier, s, ki)

    @pl.loop(ki + 1, nka)
    def _(k):
        tell(barrier, si, k)

    pbuf[...] = jnp.zeros_like(pbuf)

    pos_copy.wait()
    cls_copy.wait()
    cc_copy.wait()
    cls = clsv[...]
    charge = jnp.zeros(cls.shape, F32)
    for c in range(NCLS):
        charge = jnp.where(cls == c, jnp.broadcast_to(ccv[0:1, c : c + 1], cls.shape), charge)
    pbuf[0:3, 0:ls] = posv[...]
    pbuf[3:4, 0:ls] = charge
    x = pbuf[0:3]
    x = x - jnp.round(x)
    q = pbuf[3:4]
    x1 = x.astype(BF16).astype(F32)
    x2 = (x - x1).astype(BF16).astype(F32)
    x3 = x - x1 - x2
    half = jnp.where(q < 0.0, 0.5, 0.0)
    qc = jnp.maximum(jnp.abs(q), TINY)
    al2 = jnp.sqrt(qc)
    al = jnp.sqrt(al2)
    rows = jnp.concatenate(
        [x1, x2, x3, half, jnp.zeros((6, 128), F32), al2, al * A0, al * A1, al * A2,
         jnp.zeros((108, 128), F32)], axis=0
    )
    cols = rows.T
    own = lax.broadcasted_iota(jnp.int32, (1, 128), 1) < ls
    qown = jnp.where(own, qc, 0.0)
    tail = jnp.concatenate(
        [qown, jnp.where(own, jnp.abs(q) / qc, 0.0),
         jnp.broadcast_to(jnp.sum(qown, axis=1, keepdims=True), (1, 128)),
         jnp.zeros((5, 128), F32)], axis=0
    )
    ag_out[0:ls] = cols[0:ls]
    ag_out[ls:] = tail
    ag_in[si] = ag_out[...]

    @pl.when(si + ki > 0)
    def _():
        pl.semaphore_wait(barrier, si + ki)

    def ag_copy(src, to):
        return pltpu.make_async_remote_copy(
            src_ref=ag_out, dst_ref=ag_in.at[src], send_sem=ag_send,
            recv_sem=ag_recv.at[src], device_id=(to, ki), device_id_type=MESH,
        )

    @pl.loop(0, si)
    def _(s):
        tell(ready.at[si], s, ki)
        ag_copy(si, s).start()

    @pl.loop(0, ki)
    def _(k):
        tell(kin, si, k)

    ssin[...] = jnp.zeros_like(ssin)
    scos[...] = jnp.zeros_like(scos)
    qrow[...] = jnp.zeros_like(qrow)
    qtot[...] = jnp.zeros_like(qtot)
    facc[...] = jnp.zeros_like(facc)
    eacc[...] = jnp.zeros_like(eacc)
    mil_copy.wait()

    kbw = min(WIDE, kb)

    @pl.loop(0, n * (kb // kbw))
    def _(b):
        at = pl.ds(pl.multiple_of(b * kbw, kbw), kbw)
        m = mi[:, pl.ds(pl.multiple_of(shift * kb + b * kbw, kbw), kbw)].astype(F32)
        sq = jnp.sum(m * m, axis=0, keepdims=True)
        limit = float(MMAX * MMAX)
        wts[:, at] = limit * jnp.exp(sq * (-1.0 / limit)) / sq
        m16[:, at] = jnp.concatenate(
            [m, m, m, jnp.ones((1, kbw), F32), jnp.zeros((6, kbw), F32)], axis=0
        ).astype(BF16)

    def source(i):
        if nsite & (nsite - 1):
            return lax.rem(si + i, nsite)
        out, bit = 0, 1
        while bit < nsite:
            out = out + bit * lax.rem(lax.div(si, bit) + lax.div(i, bit), 2)
            bit *= 2
        return out

    def prepare(i):
        src = source(i)
        slot = lax.rem(i, 2)
        xs[slot] = ag_in[src, 0:ls, 0:16].astype(BF16)
        for c in range(4):
            co[slot, c] = jnp.broadcast_to(ag_in[src, 0:ls, 16 + c : 17 + c], (ls, 128))
        both = ag_in[src, ls : ls + 8]
        if nsites > 128:
            both = jnp.concatenate([both, jnp.zeros((8, nsites - 128), F32)], axis=1)
        qrow[...] += pltpu.roll(both, src * ls, 1)
        qtot[...] += ag_in[src, ls + 2 : ls + 3]

    def block_of(b):
        return pl.ds(pl.multiple_of(b * kb, kb), kb)

    prepare(0)
    tbuf[...] = jnp.dot(xs[0], m16[:, 0:kb], preferred_element_type=F32)

    def turn(i, b, slot, at_next):
        src = source(i)
        mine = lax.rem(i, 2)
        turns = jnp.dot(xs[slot], m16[:, at_next], preferred_element_type=F32)
        c0, c1, c2, c3 = co[mine, 0], co[mine, 1], co[mine, 2], co[mine, 3]
        for l in range(kb // 128):
            ln = slice(l * 128, (l + 1) * 128)
            at = pl.ds(pl.multiple_of(b * kb + l * 128, 128), 128)
            t = tbuf[:, ln]
            r = t - jnp.round(t)
            z = r * r
            s = r * (c1 + z * (c2 + z * c3))
            s2 = s * s
            u = c0 - s2
            sc = s * (u * lax.rsqrt(u))
            dc = u - s2
            sj = sc * dc
            cj = sc * sc
            psin[src, :, at] = sj
            pcos[src, :, at] = cj
            tbuf[:, ln] = turns[:, ln]
            sums, sumc = sj[0:8], cj[0:8]
            for g in range(1, ls // 8):
                sums = sums + sj[8 * g : 8 * g + 8]
                sumc = sumc + cj[8 * g : 8 * g + 8]
            ssin[:, at] += sums
            scos[:, at] += sumc

    def offer(g):
        for p, when in enumerate(offers):
            @pl.when(g == when)
            def _():
                for o in (2 * p + 1, 2 * p + 2):
                    @pl.when(si + o < nsite)
                    def _():
                        pl.semaphore_wait(ready.at[si + o], 1)
                        ag_copy(si, si + o).start()

    @pl.loop(0, nsite)
    def _(i):
        @pl.loop(0, n - 1)
        def _(b):
            offer(i * n + b)
            turn(i, b, lax.rem(i, 2), block_of(b + 1))

        offer(i * n + n - 1)

        @pl.when(i < nsite - 1)
        def _():
            nxt = source(i + 1)
            ag_copy(nxt, nxt).wait_recv()
            prepare(i + 1)

        turn(i, n - 1, lax.rem(i + 1, 2), block_of(0))

    @pl.when(ki < nka - 1)
    def _():
        pl.semaphore_wait(kin, nka - 1 - ki)

    @pl.loop(1, nka)
    def _(i):
        tell(kall, si, lax.rem(ki + i, nka))

    sent = ag_in.at[pl.ds(0, nsite - 1)]
    pltpu.make_async_copy(sent, sent, ag_send).wait()

    isn = 1.0 / math.sqrt(nsites)
    steps = n

    def step_of(j):
        return pl.ds(pl.multiple_of(j * kb, kb), kb)

    def weigh(j, counts):
        at = step_of(j)
        cimag = (4.0 * isn) * jnp.sum(ssin[:, at], axis=0, keepdims=True)
        total = jnp.concatenate([qtot[...]] * (kb // 128), axis=1)
        creal = isn * (total - 8.0 * jnp.sum(scos[:, at], axis=0, keepdims=True))
        w = wts[:, at]
        g1 = w * creal
        g2 = w * cimag
        e = g1 * creal + g2 * cimag
        eacc[...] += e if counts is None else jnp.where(counts, e, 0.0)
        g1v[...] = g1
        g2v[...] = 2.0 * g2

    weigh(0, None)

    @pl.loop(0, steps)
    def _(j):
        at = step_of(j)
        v = (psin[:, :, at] * g1v[...] + pcos[:, :, at] * g2v[...]).reshape(nsites, kb)
        hi = v.astype(BF16)
        lo = (v - hi.astype(F32)).astype(BF16)
        m = m16[:, at]
        dims = (((1,), (1,)), ((), ()))
        both = lax.dot_general(
            m, jnp.concatenate([hi, lo], axis=0), dims, preferred_element_type=F32
        )
        facc[...] += both[:, 0:nsites] + both[:, nsites:]
        weigh(jnp.minimum(j + 1, steps - 1), j + 1 < steps)

    en = eacc[:, 0:128]
    for l in range(1, kb // 128):
        en = en + eacc[:, l * 128 : (l + 1) * 128]
    if nsites > 128:
        en = jnp.concatenate([en, jnp.zeros((1, nsites - 128), F32)], axis=1)
    rs_out[...] = jnp.concatenate([facc[0:3], en], axis=0)

    pl.semaphore_wait(kall, nka - 1)

    def rs_copy(to):
        return pltpu.make_async_remote_copy(
            src_ref=rs_out, dst_ref=rs_in.at[me], send_sem=rs_send, recv_sem=rs_recv,
            device_id=(lax.div(to, nka), lax.rem(to, nka)), device_id_type=MESH,
        )

    @pl.loop(0, ndev)
    def _(to):
        @pl.when(to != me)
        def _():
            rs_copy(to).start()

    rs_in[me] = rs_out[...]
    others = rs_in.at[pl.ds(0, ndev - 1)]
    pltpu.make_async_copy(others, others, rs_recv).wait()

    total = jnp.sum(rs_in[...], axis=0)
    fall = total[0:3]
    qall, ratio = qrow[0:1], qrow[1:2]
    fscale = 16.0 * math.pi / math.sqrt(nsites * kvecs)
    mean = jnp.sum(fall, axis=1, keepdims=True) / jnp.sum(qall, axis=1, keepdims=True)
    forces = (fscale * ratio) * (fall - qall * mean)
    energy = jnp.sum(total[3:4], axis=1, keepdims=True) * (1.0 / kvecs)
    mine = pltpu.roll(
        jnp.concatenate([forces, jnp.zeros((5, nsites), F32)], axis=0), nsites - me * spd, 1
    )
    res_ref[...] = mine[:, 0:128]
    res_ref[3:4, :] = jnp.broadcast_to(energy, (1, 128))

    pltpu.make_async_copy(others, others, rs_send).wait()


def publish(res_ref, out_ref, en_ref):
    out_ref[...] = res_ref[0:3, 0 : out_ref.shape[1]]
    en_ref[...] = res_ref[3:4, 0:1]


def local(nsite, nka, positions, site_class, class_charge, miller):
    ndev = nsite * nka
    ls = positions.shape[1]
    nsites = ls * nsite
    kvecs = miller.shape[1] * nka
    spd = nsites // ndev
    kb = miller.shape[1] // (nsite * UNITS)
    span = shares(nsite, miller.shape[1] // kb)[1] * kb
    vmem = pl.BlockSpec(memory_space=pltpu.VMEM)
    summed = pl.pallas_call(
        functools.partial(kernel, nsite, nka, nsites, kvecs, kb),
        out_shape=pltpu.VMEM((8, 128), F32),
        in_specs=[pl.BlockSpec(memory_space=pl.ANY)] * 4,
        out_specs=vmem,
        scratch_shapes=[
            pltpu.VMEM((3, ls), F32),
            pltpu.VMEM((1, ls), jnp.int32),
            pltpu.VMEM((1, NCLS), F32),
            pltpu.VMEM((3, span), jnp.int32),
            pltpu.VMEM((16, span), BF16),
            pltpu.VMEM((1, span), F32),
            pltpu.VMEM((8, 128), F32),
            pltpu.VMEM((2, ls, 16), BF16),
            pltpu.VMEM((2, 4, ls, 128), F32),
            pltpu.VMEM((ls, kb), F32),
            pltpu.VMEM((nsite, ls, span), F32),
            pltpu.VMEM((nsite, ls, span), F32),
            pltpu.VMEM((8, span), F32),
            pltpu.VMEM((8, span), F32),
            pltpu.VMEM((8, nsites), F32),
            pltpu.VMEM((1, 128), F32),
            pltpu.VMEM((1, kb), F32),
            pltpu.VMEM((1, kb), F32),
            pltpu.VMEM((16, nsites), F32),
            pltpu.VMEM((1, kb), F32),
            pltpu.VMEM((ls + 8, 128), F32),
            pltpu.VMEM((nsite, ls + 8, 128), F32),
            pltpu.VMEM((4, nsites), F32),
            pltpu.VMEM((ndev, 4, nsites), F32),
            pltpu.SemaphoreType.DMA,
            pltpu.SemaphoreType.DMA,
            pltpu.SemaphoreType.DMA,
            pltpu.SemaphoreType.DMA,
            pltpu.SemaphoreType.DMA,
            pltpu.SemaphoreType.DMA((nsite,)),
            pltpu.SemaphoreType.DMA,
            pltpu.SemaphoreType.DMA,
            pltpu.SemaphoreType.REGULAR((nsite,)),
            pltpu.SemaphoreType.REGULAR,
            pltpu.SemaphoreType.REGULAR,
        ],
        compiler_params=pltpu.CompilerParams(collective_id=0, has_side_effects=True),
        name="ewald",
    )(positions, site_class.reshape(1, ls), class_charge.reshape(1, NCLS), miller)
    forces, energy = pl.pallas_call(
        publish,
        out_shape=(jax.ShapeDtypeStruct((3, spd), F32), jax.ShapeDtypeStruct((1, 1), F32)),
        in_specs=[vmem],
        out_specs=(vmem, vmem),
        name="publish",
    )(pltpu.with_memory_space_constraint(summed, pltpu.VMEM))
    return forces, energy[0, 0]


def solution(mesh):
    placed = (P(None, "site"), P("site"), P(), P(None, "ka"))
    return jax.shard_map(
        functools.partial(local, mesh.shape["site"], mesh.shape["ka"]),
        mesh=mesh,
        in_specs=placed,
        out_specs=(P(None, ("site", "ka")), P()),
        check_vma=False,
    )
```

```python
import functools
import math

import jax
import jax.numpy as jnp
from jax import lax
from jax.experimental import pallas as pl
from jax.experimental.pallas import tpu as pltpu
from jax.sharding import PartitionSpec as P

MMAX = 80
NCLS = 4
MESH = pl.DeviceIdType.MESH
F32 = jnp.float32
BF16 = jnp.bfloat16
A0, A1, A2 = 1.5707884689227576, -0.645711988911062, 0.07766738858001387
TINY = 1e-24
UNITS = 4
SKEW = (36, 8)
OFFER = (1, 3)
WIDE = 4096


def shares(nsite, units):
    total, top = SKEW[0] * nsite, SKEW[1]
    span = nsite * (total - top * nsite)

    def first(s):
        return units * s * (total - top * s) // span

    sizes = [first(s + 1) - first(s) for s in range(nsite)]
    return first, max(sizes), min(sizes)


def kernel(
    nsite, nka, nsites, kvecs, kb,
    pos_ref, cls_ref, cc_ref, mil_ref,
    res_ref,
    posv, clsv, ccv, mi, m16, wts, pbuf, xs, co, tbuf, psin, pcos, ssin, scos,
    qrow, qtot, g1v, g2v, facc, eacc,
    ag_out, ag_in, rs_out, rs_in,
    pos_sem, cls_sem, cc_sem, mil_sem, ag_send, ag_recv, rs_send, rs_recv, ready, kin, kall,
):
    ndev = nsite * nka
    si, ki = lax.axis_index("site"), lax.axis_index("ka")
    me = si * nka + ki
    ls = posv.shape[1]
    spd = nsites // ndev
    units = mil_ref.shape[1] // kb
    first, most, least = shares(nsite, units)
    offers = [min(OFFER[0] + OFFER[1] * p, nsite * least - 1) for p in range(nsite // 2)]
    low = first(si)
    n = first(si + 1) - low
    base = jnp.minimum(low, units - most)
    shift = low - base

    pos_copy = pltpu.make_async_copy(pos_ref, posv, pos_sem)
    cls_copy = pltpu.make_async_copy(cls_ref, clsv, cls_sem)
    cc_copy = pltpu.make_async_copy(cc_ref, ccv, cc_sem)
    mil_copy = pltpu.make_async_copy(
        mil_ref.at[:, pl.ds(pl.multiple_of(base * kb, 128), most * kb)], mi, mil_sem
    )
    pos_copy.start()
    cls_copy.start()
    cc_copy.start()
    mil_copy.start()

    barrier = pltpu.get_barrier_semaphore()

    def tell(sem, s, k):
        pl.semaphore_signal(sem, inc=1, device_id=(s, k), device_id_type=MESH)

    @pl.loop(si + 1, nsite)
    def _(s):
        tell(barrier, s, ki)

    @pl.loop(ki + 1, nka)
    def _(k):
        tell(barrier, si, k)

    pbuf[...] = jnp.zeros_like(pbuf)

    pos_copy.wait()
    cls_copy.wait()
    cc_copy.wait()
    cls = clsv[...]
    charge = jnp.zeros(cls.shape, F32)
    for c in range(NCLS):
        charge = jnp.where(cls == c, jnp.broadcast_to(ccv[0:1, c : c + 1], cls.shape), charge)
    pbuf[0:3, 0:ls] = posv[...]
    pbuf[3:4, 0:ls] = charge
    x = pbuf[0:3]
    x = x - jnp.round(x)
    q = pbuf[3:4]
    x1 = x.astype(BF16).astype(F32)
    x2 = (x - x1).astype(BF16).astype(F32)
    x3 = x - x1 - x2
    half = jnp.where(q < 0.0, 0.5, 0.0)
    qc = jnp.maximum(jnp.abs(q), TINY)
    al2 = jnp.sqrt(qc)
    al = jnp.sqrt(al2)
    rows = jnp.concatenate(
        [x1, x2, x3, half, jnp.zeros((6, 128), F32), al2, al * A0, al * A1, al * A2,
         jnp.zeros((108, 128), F32)], axis=0
    )
    cols = rows.T
    own = lax.broadcasted_iota(jnp.int32, (1, 128), 1) < ls
    qown = jnp.where(own, qc, 0.0)
    tail = jnp.concatenate(
        [qown, jnp.where(own, jnp.abs(q) / qc, 0.0),
         jnp.broadcast_to(jnp.sum(qown, axis=1, keepdims=True), (1, 128)),
         jnp.zeros((5, 128), F32)], axis=0
    )
    ag_out[0:ls] = cols[0:ls]
    ag_out[ls:] = tail
    ag_in[si] = ag_out[...]

    @pl.when(si + ki > 0)
    def _():
        pl.semaphore_wait(barrier, si + ki)

    def ag_copy(src, to):
        return pltpu.make_async_remote_copy(
            src_ref=ag_out, dst_ref=ag_in.at[src], send_sem=ag_send,
            recv_sem=ag_recv.at[src], device_id=(to, ki), device_id_type=MESH,
        )

    @pl.loop(0, si)
    def _(s):
        tell(ready.at[si], s, ki)
        ag_copy(si, s).start()

    @pl.loop(0, ki)
    def _(k):
        tell(kin, si, k)

    ssin[...] = jnp.zeros_like(ssin)
    scos[...] = jnp.zeros_like(scos)
    qrow[...] = jnp.zeros_like(qrow)
    qtot[...] = jnp.zeros_like(qtot)
    facc[...] = jnp.zeros_like(facc)
    eacc[...] = jnp.zeros_like(eacc)
    mil_copy.wait()

    kbw = min(WIDE, kb)

    @pl.loop(0, n * (kb // kbw))
    def _(b):
        at = pl.ds(pl.multiple_of(b * kbw, kbw), kbw)
        m = mi[:, pl.ds(pl.multiple_of(shift * kb + b * kbw, kbw), kbw)].astype(F32)
        sq = jnp.sum(m * m, axis=0, keepdims=True)
        limit = float(MMAX * MMAX)
        wts[:, at] = limit * jnp.exp(sq * (-1.0 / limit)) / sq
        m16[:, at] = jnp.concatenate(
            [m, m, m, jnp.ones((1, kbw), F32), jnp.zeros((6, kbw), F32)], axis=0
        ).astype(BF16)

    def source(i):
        if nsite & (nsite - 1):
            return lax.rem(si + i, nsite)
        out, bit = 0, 1
        while bit < nsite:
            out = out + bit * lax.rem(lax.div(si, bit) + lax.div(i, bit), 2)
            bit *= 2
        return out

    def prepare(i):
        src = source(i)
        slot = lax.rem(i, 2)
        xs[slot] = ag_in[src, 0:ls, 0:16].astype(BF16)
        for c in range(4):
            co[slot, c] = jnp.broadcast_to(ag_in[src, 0:ls, 16 + c : 17 + c], (ls, 128))
        both = ag_in[src, ls : ls + 8]
        if nsites > 128:
            both = jnp.concatenate([both, jnp.zeros((8, nsites - 128), F32)], axis=1)
        qrow[...] += pltpu.roll(both, src * ls, 1)
        qtot[...] += ag_in[src, ls + 2 : ls + 3]

    def block_of(b):
        return pl.ds(pl.multiple_of(b * kb, kb), kb)

    prepare(0)
    tbuf[...] = jnp.dot(xs[0], m16[:, 0:kb], preferred_element_type=F32)

    def turn(i, b, slot, at_next):
        src = source(i)
        mine = lax.rem(i, 2)
        turns = jnp.dot(xs[slot], m16[:, at_next], preferred_element_type=F32)
        c0, c1, c2, c3 = co[mine, 0], co[mine, 1], co[mine, 2], co[mine, 3]
        for l in range(kb // 128):
            ln = slice(l * 128, (l + 1) * 128)
            at = pl.ds(pl.multiple_of(b * kb + l * 128, 128), 128)
            t = tbuf[:, ln]
            r = t - jnp.round(t)
            z = r * r
            s = r * (c1 + z * (c2 + z * c3))
            s2 = s * s
            u = c0 - s2
            sc = s * (u * lax.rsqrt(u))
            dc = u - s2
            sj = sc * dc
            cj = sc * sc
            psin[src, :, at] = sj
            pcos[src, :, at] = cj
            tbuf[:, ln] = turns[:, ln]
            sums, sumc = sj[0:8], cj[0:8]
            for g in range(1, ls // 8):
                sums = sums + sj[8 * g : 8 * g + 8]
                sumc = sumc + cj[8 * g : 8 * g + 8]
            ssin[:, at] += sums
            scos[:, at] += sumc

    def offer(g):
        @pl.when(g <= max(offers))
        def _():
            for p, when in enumerate(offers):
                @pl.when(g == when)
                def _():
                    for o in (2 * p + 1, 2 * p + 2):
                        @pl.when(si + o < nsite)
                        def _():
                            pl.semaphore_wait(ready.at[si + o], 1)
                            ag_copy(si, si + o).start()

    @pl.loop(0, nsite)
    def _(i):
        @pl.loop(0, n - 1)
        def _(b):
            offer(i * n + b)
            turn(i, b, lax.rem(i, 2), block_of(b + 1))

        offer(i * n + n - 1)

        @pl.when(i < nsite - 1)
        def _():
            nxt = source(i + 1)
            ag_copy(nxt, nxt).wait_recv()
            prepare(i + 1)

        turn(i, n - 1, lax.rem(i + 1, 2), block_of(0))

    @pl.when(ki < nka - 1)
    def _():
        pl.semaphore_wait(kin, nka - 1 - ki)

    @pl.loop(1, nka)
    def _(i):
        tell(kall, si, lax.rem(ki + i, nka))

    sent = ag_in.at[pl.ds(0, nsite - 1)]
    pltpu.make_async_copy(sent, sent, ag_send).wait()

    isn = 1.0 / math.sqrt(nsites)
    steps = n

    def step_of(j):
        return pl.ds(pl.multiple_of(j * kb, kb), kb)

    def weigh(j, counts):
        at = step_of(j)
        cimag = (4.0 * isn) * jnp.sum(ssin[:, at], axis=0, keepdims=True)
        total = jnp.concatenate([qtot[...]] * (kb // 128), axis=1)
        creal = isn * (total - 8.0 * jnp.sum(scos[:, at], axis=0, keepdims=True))
        w = wts[:, at]
        g1 = w * creal
        g2 = w * cimag
        e = g1 * creal + g2 * cimag
        eacc[...] += e if counts is None else jnp.where(counts, e, 0.0)
        g1v[...] = g1
        g2v[...] = 2.0 * g2

    weigh(0, None)

    @pl.loop(0, steps)
    def _(j):
        at = step_of(j)
        v = (psin[:, :, at] * g1v[...] + pcos[:, :, at] * g2v[...]).reshape(nsites, kb)
        hi = v.astype(BF16)
        lo = (v - hi.astype(F32)).astype(BF16)
        m = m16[:, at]
        dims = (((1,), (1,)), ((), ()))
        both = lax.dot_general(
            m, jnp.concatenate([hi, lo], axis=0), dims, preferred_element_type=F32
        )
        facc[...] += both[:, 0:nsites] + both[:, nsites:]
        weigh(jnp.minimum(j + 1, steps - 1), j + 1 < steps)

    en = eacc[:, 0:128]
    for l in range(1, kb // 128):
        en = en + eacc[:, l * 128 : (l + 1) * 128]
    if nsites > 128:
        en = jnp.concatenate([en, jnp.zeros((1, nsites - 128), F32)], axis=1)
    rs_out[...] = jnp.concatenate([facc[0:3], en], axis=0)

    pl.semaphore_wait(kall, nka - 1)

    def rs_copy(to):
        return pltpu.make_async_remote_copy(
            src_ref=rs_out, dst_ref=rs_in.at[me], send_sem=rs_send, recv_sem=rs_recv,
            device_id=(lax.div(to, nka), lax.rem(to, nka)), device_id_type=MESH,
        )

    @pl.loop(0, ndev)
    def _(to):
        @pl.when(to != me)
        def _():
            rs_copy(to).start()

    rs_in[me] = rs_out[...]
    others = rs_in.at[pl.ds(0, ndev - 1)]
    pltpu.make_async_copy(others, others, rs_recv).wait()

    total = jnp.sum(rs_in[...], axis=0)
    fall = total[0:3]
    qall, ratio = qrow[0:1], qrow[1:2]
    fscale = 16.0 * math.pi / math.sqrt(nsites * kvecs)
    mean = jnp.sum(fall, axis=1, keepdims=True) / jnp.sum(qall, axis=1, keepdims=True)
    forces = (fscale * ratio) * (fall - qall * mean)
    energy = jnp.sum(total[3:4], axis=1, keepdims=True) * (1.0 / kvecs)
    mine = pltpu.roll(
        jnp.concatenate([forces, jnp.zeros((5, nsites), F32)], axis=0), nsites - me * spd, 1
    )
    res_ref[...] = mine[:, 0:128]
    res_ref[3:4, :] = jnp.broadcast_to(energy, (1, 128))

    pltpu.make_async_copy(others, others, rs_send).wait()


def publish(res_ref, out_ref, en_ref):
    out_ref[...] = res_ref[0:3, 0 : out_ref.shape[1]]
    en_ref[...] = res_ref[3:4, 0:1]


def local(nsite, nka, positions, site_class, class_charge, miller):
    ndev = nsite * nka
    ls = positions.shape[1]
    nsites = ls * nsite
    kvecs = miller.shape[1] * nka
    spd = nsites // ndev
    kb = miller.shape[1] // (nsite * UNITS)
    span = shares(nsite, miller.shape[1] // kb)[1] * kb
    vmem = pl.BlockSpec(memory_space=pltpu.VMEM)
    summed = pl.pallas_call(
        functools.partial(kernel, nsite, nka, nsites, kvecs, kb),
        out_shape=pltpu.VMEM((8, 128), F32),
        in_specs=[pl.BlockSpec(memory_space=pl.ANY)] * 4,
        out_specs=vmem,
        scratch_shapes=[
            pltpu.VMEM((3, ls), F32),
            pltpu.VMEM((1, ls), jnp.int32),
            pltpu.VMEM((1, NCLS), F32),
            pltpu.VMEM((3, span), jnp.int32),
            pltpu.VMEM((16, span), BF16),
            pltpu.VMEM((1, span), F32),
            pltpu.VMEM((8, 128), F32),
            pltpu.VMEM((2, ls, 16), BF16),
            pltpu.VMEM((2, 4, ls, 128), F32),
            pltpu.VMEM((ls, kb), F32),
            pltpu.VMEM((nsite, ls, span), F32),
            pltpu.VMEM((nsite, ls, span), F32),
            pltpu.VMEM((8, span), F32),
            pltpu.VMEM((8, span), F32),
            pltpu.VMEM((8, nsites), F32),
            pltpu.VMEM((1, 128), F32),
            pltpu.VMEM((1, kb), F32),
            pltpu.VMEM((1, kb), F32),
            pltpu.VMEM((16, nsites), F32),
            pltpu.VMEM((1, kb), F32),
            pltpu.VMEM((ls + 8, 128), F32),
            pltpu.VMEM((nsite, ls + 8, 128), F32),
            pltpu.VMEM((4, nsites), F32),
            pltpu.VMEM((ndev, 4, nsites), F32),
            pltpu.SemaphoreType.DMA,
            pltpu.SemaphoreType.DMA,
            pltpu.SemaphoreType.DMA,
            pltpu.SemaphoreType.DMA,
            pltpu.SemaphoreType.DMA,
            pltpu.SemaphoreType.DMA((nsite,)),
            pltpu.SemaphoreType.DMA,
            pltpu.SemaphoreType.DMA,
            pltpu.SemaphoreType.REGULAR((nsite,)),
            pltpu.SemaphoreType.REGULAR,
            pltpu.SemaphoreType.REGULAR,
        ],
        compiler_params=pltpu.CompilerParams(collective_id=0, has_side_effects=True),
        name="ewald",
    )(positions, site_class.reshape(1, ls), class_charge.reshape(1, NCLS), miller)
    forces, energy = pl.pallas_call(
        publish,
        out_shape=(jax.ShapeDtypeStruct((3, spd), F32), jax.ShapeDtypeStruct((1, 1), F32)),
        in_specs=[vmem],
        out_specs=(vmem, vmem),
        name="publish",
    )(pltpu.with_memory_space_constraint(summed, pltpu.VMEM))
    return forces, energy[0, 0]


def solution(mesh):
    placed = (P(None, "site"), P("site"), P(), P(None, "ka"))
    return jax.shard_map(
        functools.partial(local, mesh.shape["site"], mesh.shape["ka"]),
        mesh=mesh,
        in_specs=placed,
        out_specs=(P(None, ("site", "ka")), P()),
        check_vma=False,
    )
```
